32 devices in a mesh: dp: 4 (over y, z), ep: 8 (over x, core).
Axes of the slice: x: 4, y: 2, z: 2, core: 2. Of those that a mesh axis runs over, the one named last changes fastest.
The devices are a block of a 4x4x8 slice.
Arguments:
- tokens: bfloat16 [8192, 1024], P(('dp', 'ep')), parts along dimension 0
- expert_ids: int32 [8192, 8], P(('dp', 'ep')), parts along dimension 0
- gate_vals: float32 [8192, 8], P(('dp', 'ep')), parts along dimension 0
- w_gate: bfloat16 [32, 1024, 512], P('ep')
- w_up: bfloat16 [32, 1024, 512], P('ep')
- w_down: bfloat16 [32, 512, 1024], P('ep')
Outputs:
- output: bfloat16 [8192, 1024], P(('dp', 'ep')), parts along dimension 0
There are 4 independent parts. The reference program is written for one: setup_inputs(seed, part) draws one part's arguments, and reference() takes and returns one part's arrays. A program takes and returns all parts, laid end to end along the dimension named above; an argument that names none is the same for every part.
All inputs are finite; a program needn't handle non-finite values.
Results may differ from the reference program's by a relative error of at most 0.00631461.
Values are sent between devices in bfloat16 or wider.
A program may use at most 768 MiB of HBM per device.

```python
import jax
import jax.numpy as jnp
from jax import lax

D_MODEL = 1024
FFN_DIM = 512
NUM_EXPERTS = 32
TOP_K = 8
GROUP = 8
TOK_DEV = 256

DEV_LIMIT = TOP_K // 2
LOCAL_EXPERTS = NUM_EXPERTS // GROUP
PAIR_CAP = TOK_DEV * DEV_LIMIT // GROUP
EXPERT_CAP = TOK_DEV * TOP_K * GROUP // NUM_EXPERTS
TOKENS = GROUP * TOK_DEV


def perm_rows(rand_key, row_count, perm_size):
    return jax.vmap(lambda sub_key: jax.random.permutation(sub_key, perm_size))(jax.random.split(rand_key, row_count))


def draw_routing(rand_key):
    key_src, key_dst, key_slot = jax.random.split(rand_key, 3)
    src_perm = perm_rows(key_src, GROUP, GROUP)
    dst_perm = perm_rows(key_dst, GROUP, LOCAL_EXPERTS)
    flat_pos = jnp.arange(TOK_DEV)[:, None] * DEV_LIMIT + jnp.arange(DEV_LIMIT)[None, :]
    dest_dev = src_perm[:, flat_pos % GROUP]
    recv_row = jnp.arange(GROUP)[:, None, None] * PAIR_CAP + (flat_pos // GROUP)[None, :, :]
    first_loc = dst_perm[dest_dev, (2 * recv_row) % LOCAL_EXPERTS]
    second_loc = dst_perm[dest_dev, (2 * recv_row + 1) % LOCAL_EXPERTS]
    pair_ids = jnp.stack([first_loc, second_loc], axis=-1) + dest_dev[..., None] * LOCAL_EXPERTS
    ordered = pair_ids.reshape(TOKENS, TOP_K)
    scores = jax.random.randint(key_slot, (TOKENS, TOP_K), 0, 1 << 20) * TOP_K + jnp.arange(TOP_K)[None, :]
    slot_order = jnp.argsort(scores, axis=1)
    return jnp.take_along_axis(ordered, slot_order, axis=1).astype(jnp.int32)


def setup_inputs(seed: int = 0, part: int = 0) -> dict:
    base_key = jax.random.key(seed)
    key_x, key_route, key_gate = jax.random.split(jax.random.fold_in(base_key, part), 3)
    key_wg, key_wu, key_wd = jax.random.split(jax.random.key(seed + 1), 3)
    in_scale = D_MODEL ** -0.5
    out_scale = 2.0 * FFN_DIM ** -0.5
    tokens = jax.random.normal(key_x, (TOKENS, D_MODEL), jnp.float32).astype(jnp.bfloat16)
    expert_ids = draw_routing(key_route)
    logits = 1.5 * jax.random.normal(key_gate, (TOKENS, TOP_K), jnp.float32)
    gate_vals = jax.nn.softmax(logits, axis=-1)
    w_gate = (in_scale * jax.random.normal(key_wg, (NUM_EXPERTS, D_MODEL, FFN_DIM), jnp.float32)).astype(jnp.bfloat16)
    w_up = (in_scale * jax.random.normal(key_wu, (NUM_EXPERTS, D_MODEL, FFN_DIM), jnp.float32)).astype(jnp.bfloat16)
    w_down = (out_scale * jax.random.normal(key_wd, (NUM_EXPERTS, FFN_DIM, D_MODEL), jnp.float32)).astype(jnp.bfloat16)
    return {'tokens': tokens, 'expert_ids': expert_ids, 'gate_vals': gate_vals, 'w_gate': w_gate, 'w_up': w_up, 'w_down': w_down}


def expert_ffn(row_in, gate_mat, up_mat, down_mat):
    gate_act = jnp.dot(row_in, gate_mat, preferred_element_type=jnp.float32)
    up_act = jnp.dot(row_in, up_mat, preferred_element_type=jnp.float32)
    hidden = (jax.nn.silu(gate_act) * up_act).astype(jnp.bfloat16)
    return jnp.dot(hidden, down_mat, preferred_element_type=jnp.float32).astype(jnp.bfloat16)


def reference(tokens, expert_ids, gate_vals, w_gate, w_up, w_down):
    pair_count = TOKENS * TOP_K
    flat_ids = expert_ids.reshape(pair_count)
    pair_index = jnp.arange(pair_count, dtype=jnp.int32)

    def one_expert(map_item):
        expert, gate_mat, up_mat, down_mat = map_item
        member = flat_ids == expert
        slot_pos = jnp.where(member, jnp.cumsum(member.astype(jnp.int32)) - 1, EXPERT_CAP)
        pair_list = jnp.full((EXPERT_CAP,), pair_count, jnp.int32).at[slot_pos].set(pair_index, mode='drop')
        row_in = tokens[jnp.minimum(pair_list, pair_count - 1) // TOP_K]
        return pair_list, expert_ffn(row_in, gate_mat, up_mat, down_mat)

    pair_lists, expert_rows = lax.map(one_expert, (jnp.arange(NUM_EXPERTS, dtype=jnp.int32), w_gate, w_up, w_down))
    pair_out = jnp.zeros((pair_count, D_MODEL), jnp.bfloat16).at[pair_lists.reshape(-1)].set(expert_rows.reshape(-1, D_MODEL), mode='drop')
    earlier = jnp.arange(TOP_K)[None, :] < jnp.arange(TOP_K)[:, None]

    def combine_block(blk_item):
        rows_in, ids_in, gate_in, outs_in = blk_item
        dev_of = ids_in // LOCAL_EXPERTS
        same_dev = dev_of[:, :, None] == dev_of[:, None, :]
        weights = jnp.where(same_dev, gate_in[:, None, :], 0.0)
        dev_sum = jnp.einsum('tjk,tkd->tjd', weights, outs_in.astype(jnp.float32)).astype(jnp.bfloat16)
        leader = jnp.logical_not(jnp.any(same_dev & earlier[None, :, :], axis=2))
        moe_sum = jnp.sum(jnp.where(leader[:, :, None], dev_sum.astype(jnp.float32), 0.0), axis=1)
        return (rows_in.astype(jnp.float32) + moe_sum).astype(jnp.bfloat16)

    output = lax.map(combine_block, (tokens.reshape(GROUP, TOK_DEV, D_MODEL), expert_ids.reshape(GROUP, TOK_DEV, TOP_K), gate_vals.reshape(GROUP, TOK_DEV, TOP_K), pair_out.reshape(GROUP, TOK_DEV, TOP_K, D_MODEL)))
    return output.reshape(TOKENS, D_MODEL)
```

```python
import functools

import jax
import jax.numpy as jnp
from jax import lax
from jax.experimental import pallas as pl
from jax.experimental.pallas import tpu as pltpu
from jax.sharding import PartitionSpec as P

MESH = pl.DeviceIdType.MESH
F32, BF16 = jnp.float32, jnp.bfloat16
OWN, MATE, R0, R1, O0, O1, L0, L1 = range(8)


def back(slot):
    return (-(slot // 2)) % 4 * 2 + slot % 2


def kernel(tok, ids, gates, wg_hbm, wu_hbm, wd_hbm, out,
           xs, tables, mytab, tri, wg, wu, wd, sums, home, acc, rank_home,
           tok_sem, w_sem, xs_send, xs_recv, tab_send, tab_recv, s_send, s_recv):
    rows, half = tok.shape[0], tok.shape[0] // 2
    n_exp = wg.shape[0]
    me = lax.axis_index("ep")
    x = me // 2
    c = me - 2 * x
    x_of = [lax.rem(x + d, 4) for d in range(4)]
    dev = [2 * x_of[s // 2] + (1 - c if s % 2 else c) for s in range(8)]

    def remote(src, dst, send, recv, slot):
        return pltpu.make_async_remote_copy(src_ref=src, dst_ref=dst, send_sem=send, recv_sem=recv,
                                            device_id={"ep": dev[slot]}, device_id_type=MESH)

    tok_in = pltpu.make_async_copy(tok, xs.at[OWN], tok_sem)
    tok_in.start()
    weights = [[pltpu.make_async_copy(h.at[e], v.at[e], w_sem.at[i, e]) for i, (h, v) in
                enumerate(((wg_hbm, wg), (wu_hbm, wu), (wd_hbm, wd)))] for e in range(n_exp)]
    for e in range(n_exp):
        for cp in weights[e]:
            cp.start()

    barrier = pltpu.get_barrier_semaphore()
    for s in range(1, 8):
        pl.semaphore_signal(barrier, inc=1, device_id={"ep": dev[s]}, device_id_type=MESH)
    pl.semaphore_wait(barrier, 7)
    tok_in.wait()

    halves = (pl.ds(0, half), pl.ds(half, half))

    def block(slot_src, h, to, sem):
        owner = (slot_src // 2 - to // 2) % 4 * 2 + (slot_src % 2 + to % 2) % 2
        return remote(xs.at[slot_src, halves[h]], xs.at[owner, halves[h]], xs_send.at[sem], xs_recv.at[owner, h], to)

    sends = []

    def go(cp):
        cp.start()
        sends.append(cp)

    def arrived(slot, h):
        pltpu.make_async_remote_copy(src_ref=xs.at[slot, halves[h]], dst_ref=xs.at[slot, halves[h]], send_sem=xs_send.at[0],
                                     recv_sem=xs_recv.at[slot, h], device_id={"ep": dev[MATE]},
                                     device_id_type=MESH).wait_recv()

    go(block(OWN, 0, R0, 0))
    go(block(OWN, 1, L0, 1))
    go(block(OWN, 1, R0, 2))
    go(block(OWN, 0, L0, 3))
    go(block(OWN, 0, MATE, 4))
    go(block(OWN, 1, MATE, 5))

    row8 = lax.broadcasted_iota(jnp.int32, (2 * n_exp, half), 0)
    in_first = row8 < n_exp
    exp_of = jnp.where(in_first, row8, row8 - n_exp)
    id_rep = [jnp.where(in_first, ids[j:j + 1, 0:half], ids[j:j + 1, half:rows]) for j in range(ids.shape[0])]
    g_rep = [jnp.where(in_first, gates[j:j + 1, 0:half], gates[j:j + 1, half:rows]) for j in range(ids.shape[0])]
    for s in range(8):
        want = exp_of + dev[s] * n_exp
        tab = jnp.zeros((2 * n_exp, half), F32)
        for j in range(ids.shape[0]):
            tab = tab + jnp.where(id_rep[j] == want, g_rep[j], 0.0)
        mytab[s] = tab
    for i, s in enumerate((MATE, R0, L0, R1, L1, O0, O1)):
        go(remote(mytab.at[s], tables.at[back(s)], tab_send.at[i], tab_recv.at[back(s)], s))

    def table_arrived(slot):
        pltpu.make_async_remote_copy(src_ref=tables.at[slot], dst_ref=tables.at[slot], send_sem=tab_send.at[0],
                                     recv_sem=tab_recv.at[slot], device_id={"ep": dev[MATE]},
                                     device_id_type=MESH).wait_recv()

    tri[...] = (lax.broadcasted_iota(jnp.int32, (rows, rows), 0) <=
                lax.broadcasted_iota(jnp.int32, (rows, rows), 1)).astype(F32).astype(BF16)

    def place(tab):
        hit = (tab != 0.0).astype(F32)
        one = [jnp.max(hit[i * n_exp:(i + 1) * n_exp], axis=0, keepdims=True) for i in range(2)]
        hit = jnp.concatenate(one, axis=1)
        count = jnp.dot(jnp.broadcast_to(hit, (16, rows)).astype(BF16), tri[...], preferred_element_type=F32)[0:1]
        return jnp.where(hit > 0.0, count - 1.0, -1.0)

    def one_hot(where):
        slot_row = lax.broadcasted_iota(jnp.int32, (half, rows), 0).astype(F32)
        return (slot_row == where).astype(F32)

    for s in range(8):
        rank_home[s:s + 1] = place(mytab[s])

    def serve(slot, first=False):
        tab = mytab[OWN] if slot == OWN else tables[slot]
        pick = one_hot(place(tab))
        row_in = jnp.dot(pick.astype(BF16), xs[slot], preferred_element_type=F32).astype(BF16)
        part = [lax.dot_general(pick[:, i * half:(i + 1) * half], tab, (((1,), (1,)), ((), ())),
                                precision=lax.Precision.HIGHEST, preferred_element_type=F32) for i in range(2)]
        total = jnp.zeros((half, xs.shape[2]), F32)
        for e in range(n_exp):
            if first:
                for cp in weights[e]:
                    cp.wait()
            a = jnp.dot(row_in, wg[e], preferred_element_type=F32)
            b = jnp.dot(row_in, wu[e], preferred_element_type=F32)
            hid = (a * (1.0 / (1.0 + jnp.exp(-a))) * b).astype(BF16)
            y = jnp.dot(hid, wd[e], preferred_element_type=F32).astype(BF16).astype(F32)
            g = part[0][:, e:e + 1] + part[1][:, n_exp + e:n_exp + e + 1]
            total = total + jnp.where(g != 0.0, g * y, 0.0)
        return total.astype(BF16)

    def answer(slot):
        sums[slot] = serve(slot)
        go(remote(sums.at[slot], home.at[back(slot)], s_send.at[slot], s_recv.at[back(slot)], slot))

    home[OWN] = serve(OWN, first=True)
    for h in range(2):
        arrived(MATE, h)
    table_arrived(MATE)
    answer(MATE)
    arrived(L0, 0)
    go(block(L0, 0, R0, 6))
    go(block(L0, 0, MATE, 8))
    arrived(R0, 1)
    go(block(R0, 1, L0, 7))
    go(block(R0, 1, MATE, 9))
    arrived(L0, 1)
    go(block(L0, 1, MATE, 10))
    arrived(R0, 0)
    go(block(R0, 0, MATE, 11))
    table_arrived(L0)
    answer(L0)
    table_arrived(R0)
    answer(R0)
    for h in range(2):
        arrived(L1, h)
    table_arrived(L1)
    answer(L1)
    for h in range(2):
        arrived(O0, h)
        go(block(O0, h, MATE, 12 + h))
    for h in range(2):
        arrived(R1, h)
    table_arrived(R1)
    answer(R1)
    table_arrived(O0)
    answer(O0)
    for h in range(2):
        arrived(O1, h)
    table_arrived(O1)
    answer(O1)

    def back_home(pair):
        pick = jnp.concatenate([one_hot(rank_home[2 * pair + i:2 * pair + i + 1]) for i in range(2)], axis=0).astype(BF16)
        got = home[pl.ds(2 * pair, 2)].reshape(rows, home.shape[2])
        return lax.dot_general(pick, got, (((0,), (0,)), ((), ())), preferred_element_type=F32)

    def sum_arrived(slot):
        pltpu.make_async_remote_copy(src_ref=home.at[slot], dst_ref=home.at[slot], send_sem=s_send.at[0],
                                     recv_sem=s_recv.at[slot], device_id={"ep": dev[MATE]},
                                     device_id_type=MESH).wait_recv()

    sum_arrived(MATE)
    acc[...] = xs[OWN].astype(F32) + back_home(0)
    for s in (L0, L1):
        sum_arrived(s)
    acc[...] += back_home(3)
    for s in (R0, R1):
        sum_arrived(s)
    acc[...] += back_home(1)
    for s in (O0, O1):
        sum_arrived(s)
    out[...] = (acc[...] + back_home(2)).astype(BF16)
    for cp in sends:
        cp.wait_send()


def solution(mesh):
    row_spec = P(('dp', 'ep'))
    expert_spec = P('ep')
    group = mesh.shape['ep']
    assert group == 8

    def device_step(tokens, expert_ids, gate_vals, w_gate, w_up, w_down):
        rows, width = tokens.shape
        n_exp, _, hidden = w_gate.shape
        half = rows // 2
        any_spec = pl.BlockSpec(memory_space=pl.ANY)
        vmem_spec = pl.BlockSpec(memory_space=pltpu.VMEM)
        dma = pltpu.SemaphoreType.DMA
        return pl.pallas_call(
            kernel,
            out_shape=jax.ShapeDtypeStruct((rows, width), BF16),
            in_specs=[any_spec, vmem_spec, vmem_spec, any_spec, any_spec, any_spec],
            out_specs=vmem_spec,
            scratch_shapes=[
                pltpu.VMEM((group, rows, width), BF16),
                pltpu.VMEM((group, 2 * n_exp, half), F32),
                pltpu.VMEM((group, 2 * n_exp, half), F32),
                pltpu.VMEM((rows, rows), BF16),
                pltpu.VMEM((n_exp, width, hidden), BF16),
                pltpu.VMEM((n_exp, width, hidden), BF16),
                pltpu.VMEM((n_exp, hidden, width), BF16),
                pltpu.VMEM((group, half, width), BF16),
                pltpu.VMEM((group, half, width), BF16),
                pltpu.VMEM((rows, width), F32),
                pltpu.VMEM((group, rows), F32),
                dma, dma((3, n_exp)), dma((14,)), dma((group, 2)), dma((7,)), dma((group,)), dma((group,)), dma((group,)),
            ],
            compiler_params=pltpu.CompilerParams(collective_id=0, has_side_effects=True, vmem_limit_bytes=60 * 1024 * 1024),
        )(tokens, expert_ids.T, gate_vals.T, w_gate, w_up, w_down)

    return jax.shard_map(device_step, mesh=mesh, in_specs=(row_spec, row_spec, row_spec, expert_spec, expert_spec, expert_spec),
                         out_specs=row_spec, check_vma=False)
```

```python
import functools

import jax
import jax.numpy as jnp
from jax import lax
from jax.experimental import pallas as pl
from jax.experimental.pallas import tpu as pltpu
from jax.sharding import PartitionSpec as P

MESH = pl.DeviceIdType.MESH
F32, BF16 = jnp.float32, jnp.bfloat16
OWN, MATE, A0, B0, A1, B1, O0, O1 = range(8)
CHIP = (0, 0, 1, 3, 1, 3, 2, 2)
CORE = (0, 1, 0, 0, 1, 1, 0, 1)


def seen_from(owner, reader):
    want = (CHIP[owner] ^ CHIP[reader], CORE[owner] ^ CORE[reader])
    return [s for s in range(8) if (CHIP[s], CORE[s]) == want][0]


def kernel(tok, ids_hbm, gates_hbm, wg_hbm, wu_hbm, wd_hbm, out,
           xs, tables, mytab, tri, wgu, wd, row_in, sums, home, acc, rank_home, ids, gates,
           tok_sem, route_sem, w_sem, xs_send, tab_send, s_send, xs_recv, half_recv, tab_recv, s_recv):
    rows, half = tok.shape[0], tok.shape[0] // 2
    n_exp = wd.shape[0]
    me = lax.axis_index("ep")
    x = me // 2
    c = me - 2 * x
    x_of = (x, x + 1 - 2 * lax.rem(x, 2), lax.rem(x + 2, 4), 3 - x)
    dev = [2 * x_of[CHIP[s]] + (1 - c if CORE[s] else c) for s in range(8)]

    def remote(src, dst, send, recv, slot):
        return pltpu.make_async_remote_copy(src_ref=src, dst_ref=dst, send_sem=send, recv_sem=recv,
                                            device_id={"ep": dev[slot]}, device_id_type=MESH)

    def wait_for(ref, sem):
        remote(ref, ref, xs_send, sem, MATE).wait_recv()

    tok_in = pltpu.make_async_copy(tok, xs.at[OWN], tok_sem)
    tok_in.start()
    route_in = [pltpu.make_async_copy(h, v, route_sem.at[i]) for i, (h, v) in enumerate(((ids_hbm, ids), (gates_hbm, gates)))]
    for cp in route_in:
        cp.start()
    barrier = pltpu.get_barrier_semaphore()
    for s in range(1, 8):
        pl.semaphore_signal(barrier, inc=1, device_id={"ep": dev[s]}, device_id_type=MESH)
    pl.semaphore_wait(barrier, 7)
    tok_in.wait()

    part = (pl.ds(0, half), pl.ds(half, half))
    whole = pl.ds(0, rows)

    def pass_on(owner, h, to, recv):
        slot = seen_from(owner, to)
        remote(xs.at[owner, h], xs.at[slot, h], xs_send, recv, to).start()

    for i in range(2):
        pass_on(OWN, part[i], A0, half_recv.at[0, i])
        pass_on(OWN, part[1 - i], B0, half_recv.at[1, i])
    pass_on(OWN, whole, MATE, xs_recv.at[MATE])
    w_in = [pltpu.make_async_copy(wg_hbm, wgu.at[0], w_sem.at[0]), pltpu.make_async_copy(wu_hbm, wgu.at[1], w_sem.at[0]),
            pltpu.make_async_copy(wd_hbm, wd, w_sem.at[1])]
    for cp in w_in:
        cp.start()

    for cp in route_in:
        cp.wait()
    row8 = lax.broadcasted_iota(jnp.int32, (2 * n_exp, half), 0)
    in_first = row8 < n_exp
    exp_of = jnp.where(in_first, row8, row8 - n_exp)
    id_rep = [jnp.where(in_first, ids[j:j + 1, 0:half], ids[j:j + 1, half:rows]) for j in range(ids.shape[0])]
    g_rep = [jnp.where(in_first, gates[j:j + 1, 0:half], gates[j:j + 1, half:rows]) for j in range(ids.shape[0])]
    for s in range(8):
        want = exp_of + dev[s] * n_exp
        tab = jnp.zeros((2 * n_exp, half), F32)
        for j in range(ids.shape[0]):
            tab = tab + jnp.where(id_rep[j] == want, g_rep[j], 0.0)
        mytab[s] = tab
    tri[...] = (lax.broadcasted_iota(jnp.int32, (rows, rows), 0) <=
                lax.broadcasted_iota(jnp.int32, (rows, rows), 1)).astype(F32).astype(BF16)
    for s in range(1, 8):
        remote(mytab.at[s], tables.at[s], tab_send, tab_recv.at[s // 2], s).start()

    def place(tab):
        hit = (tab != 0.0).astype(F32)
        one = [jnp.max(hit[i * n_exp:(i + 1) * n_exp], axis=0, keepdims=True) for i in range(2)]
        hit = jnp.concatenate(one, axis=1)
        count = jnp.dot(jnp.broadcast_to(hit, (16, rows)).astype(BF16), tri[...], preferred_element_type=F32)[0:1]
        return jnp.where(hit > 0.0, count - 1.0, -1.0)

    def one_hot(where):
        slot_row = lax.broadcasted_iota(jnp.int32, (half, rows), 0).astype(F32)
        return (slot_row == where).astype(F32)

    for s in range(8):
        rank_home[s:s + 1] = place(mytab[s])

    def serve(pair):
        weight = []
        for i, slot in enumerate(pair):
            tab = mytab[OWN] if slot == OWN else tables[slot]
            pick = one_hot(rank_home[OWN:OWN + 1] if slot == OWN else place(tab))
            row_in[part[i], :] = jnp.dot(pick.astype(BF16), xs[slot], preferred_element_type=F32).astype(BF16)
            g = [lax.dot_general(pick[:, j * half:(j + 1) * half], tab, (((1,), (1,)), ((), ())),
                                 precision=lax.Precision.HIGHEST, preferred_element_type=F32) for j in range(2)]
            weight.append([g[0][:, e:e + 1] + g[1][:, n_exp + e:n_exp + e + 1] for e in range(n_exp)])
        total = jnp.zeros(acc.shape, F32)
        for e in range(n_exp):
            a = jnp.dot(row_in[...], wgu[0, e], preferred_element_type=F32)
            b = jnp.dot(row_in[...], wgu[1, e], preferred_element_type=F32)
            hid = (a * (1.0 / (1.0 + jnp.exp(-a))) * b).astype(BF16)
            y = jnp.dot(hid, wd[e], preferred_element_type=F32).astype(BF16).astype(F32)
            g = jnp.concatenate([w[e] for w in weight], axis=0)
            total = total + jnp.where(g != 0.0, g * y, 0.0)
        total = total.astype(BF16)
        for i, slot in enumerate(pair):
            (home if slot == OWN else sums)[slot] = total[i * half:(i + 1) * half]
        for slot in pair:
            if slot != OWN:
                remote(sums.at[slot], home.at[slot], s_send, s_recv.at[slot // 2], slot).start()

    def tables_of(pair):
        wait_for(tables.at[pl.ds(pair[0], 2)] if pair[0] else tables.at[MATE], tab_recv.at[pair[0] // 2])

    wait_for(xs.at[MATE], xs_recv.at[MATE])
    tables_of((OWN, MATE))
    wait_for(wgu, w_sem.at[0])
    w_in[2].wait()
    serve((OWN, MATE))
    for slot, on, i in ((A0, B0, 0), (B0, A0, 1)):
        wait_for(xs.at[slot, part[i]], half_recv.at[i, 0])
        pass_on(slot, part[i], on, xs_recv.at[O0])
        pass_on(slot, part[i], MATE, xs_recv.at[seen_from(slot, MATE)])
    for slot, i in ((A0, 0), (B0, 1)):
        wait_for(xs.at[slot, part[1 - i]], half_recv.at[i, 1])
        pass_on(slot, part[1 - i], MATE, xs_recv.at[seen_from(slot, MATE)])
    tables_of((A0, B0))
    serve((A0, B0))
    wait_for(xs.at[A1], xs_recv.at[A1])
    wait_for(xs.at[B1], xs_recv.at[B1])
    tables_of((A1, B1))
    serve((A1, B1))
    wait_for(xs.at[O0], xs_recv.at[O0])
    pass_on(O0, whole, MATE, xs_recv.at[O1])
    wait_for(xs.at[O1], xs_recv.at[O1])
    tables_of((O0, O1))
    serve((O0, O1))

    def back_home(pair):
        pick = jnp.concatenate([one_hot(rank_home[s:s + 1]) for s in (pair, pair + 1)], axis=0).astype(BF16)
        got = home[pl.ds(pair, 2)].reshape(rows, home.shape[2])
        return lax.dot_general(pick, got, (((0,), (0,)), ((), ())), preferred_element_type=F32)

    wait_for(home.at[MATE], s_recv.at[0])
    acc[...] = xs[OWN].astype(F32) + back_home(OWN)
    for pair in (A0, A1):
        wait_for(home.at[pl.ds(pair, 2)], s_recv.at[pair // 2])
        acc[...] += back_home(pair)
    wait_for(home.at[pl.ds(O0, 2)], s_recv.at[O0 // 2])
    out[...] = (acc[...] + back_home(O0)).astype(BF16)
    for ref, sem in ((xs, xs_send), (mytab, tab_send), (sums, s_send)):
        remote(ref.at[pl.ds(0, 7)], ref.at[pl.ds(0, 7)], sem, s_recv.at[0], MATE).wait_send()


def solution(mesh):
    row_spec = P(('dp', 'ep'))
    expert_spec = P('ep')
    group = mesh.shape['ep']
    assert group == 8

    def device_step(tokens, expert_ids, gate_vals, w_gate, w_up, w_down):
        rows, width = tokens.shape
        n_exp, _, hidden = w_gate.shape
        half = rows // 2
        in_hbm = functools.partial(pltpu.with_memory_space_constraint, memory_space=pltpu.HBM)
        dma = pltpu.SemaphoreType.DMA
        return pl.pallas_call(
            kernel,
            out_shape=jax.ShapeDtypeStruct((rows, width), BF16),
            in_specs=[pl.BlockSpec(memory_space=pltpu.HBM)] * 6,
            out_specs=pl.BlockSpec(memory_space=pltpu.VMEM),
            scratch_shapes=[
                pltpu.VMEM((group, rows, width), BF16),
                pltpu.VMEM((group, 2 * n_exp, half), F32),
                pltpu.VMEM((group, 2 * n_exp, half), F32),
                pltpu.VMEM((rows, rows), BF16),
                pltpu.VMEM((2, n_exp, width, hidden), BF16),
                pltpu.VMEM((n_exp, hidden, width), BF16),
                pltpu.VMEM((rows, width), BF16),
                pltpu.VMEM((group, half, width), BF16),
                pltpu.VMEM((group, half, width), BF16),
                pltpu.VMEM((rows, width), F32),
                pltpu.VMEM((group, rows), F32),
                pltpu.VMEM((expert_ids.shape[1], rows), jnp.int32),
                pltpu.VMEM((expert_ids.shape[1], rows), F32),
                dma, dma((2,)), dma((2,)), dma, dma, dma, dma((group,)), dma((2, 2)), dma((4,)), dma((4,)),
            ],
            compiler_params=pltpu.CompilerParams(collective_id=0, has_side_effects=True, vmem_limit_bytes=40 * 1024 * 1024),
        )(*map(in_hbm, (tokens, expert_ids.T, gate_vals.T, w_gate, w_up, w_down)))

    return jax.shard_map(device_step, mesh=mesh, in_specs=(row_spec, row_spec, row_spec, expert_spec, expert_spec, expert_spec),
                         out_specs=row_spec, check_vma=False)
```

```python
import functools

import jax
import jax.numpy as jnp
from jax import lax
from jax.experimental import pallas as pl
from jax.experimental.pallas import tpu as pltpu
from jax.sharding import PartitionSpec as P

MESH = pl.DeviceIdType.MESH
F32, BF16 = jnp.float32, jnp.bfloat16
OWN, MATE, A0, B0, A1, B1, O0, O1 = range(8)
CHIP = (0, 0, 1, 3, 1, 3, 2, 2)
CORE = (0, 1, 0, 0, 1, 1, 0, 1)


def seen_from(owner, reader):
    want = (CHIP[owner] ^ CHIP[reader], CORE[owner] ^ CORE[reader])
    return [s for s in range(8) if (CHIP[s], CORE[s]) == want][0]


def kernel(tok, ids_hbm, gates_hbm, wg_hbm, wu_hbm, wd_hbm, out,
           xs, tables, mytab, tri, wgu, wd, row_in, sums, home, acc, rank_home, ids, gates, pick, weight,
           tok_sem, route_sem, w_sem, xs_send, tab_send, s_send, xs_recv, half_recv, tab_recv, s_recv, arrived):
    rows, half = tok.shape[0], tok.shape[0] // 2
    n_exp = wd.shape[0]
    me = lax.axis_index("ep")
    x = me // 2
    c = me - 2 * x
    x_of = (x, x + 1 - 2 * lax.rem(x, 2), lax.rem(x + 2, 4), 3 - x)
    dev = [2 * x_of[CHIP[s]] + (1 - c if CORE[s] else c) for s in range(8)]

    def remote(src, dst, send, recv, slot):
        return pltpu.make_async_remote_copy(src_ref=src, dst_ref=dst, send_sem=send, recv_sem=recv,
                                            device_id={"ep": dev[slot]}, device_id_type=MESH)

    def wait_for(ref, sem):
        remote(ref, ref, xs_send, sem, MATE).wait_recv()

    tok_in = pltpu.make_async_copy(tok, xs.at[OWN], tok_sem)
    tok_in.start()
    route_in = [pltpu.make_async_copy(h, v, route_sem.at[i]) for i, (h, v) in enumerate(((ids_hbm, ids), (gates_hbm, gates)))]
    for cp in route_in:
        cp.start()
    barrier = pltpu.get_barrier_semaphore()
    for s in (A0, B0, MATE):
        pl.semaphore_signal(barrier, inc=1, device_id={"ep": dev[s]}, device_id_type=MESH)
    pl.semaphore_wait(barrier, 3)
    for s in (A0, B0):
        pl.semaphore_signal(arrived.at[0], inc=1, device_id={"ep": dev[s]}, device_id_type=MESH)
    tok_in.wait()

    part = (pl.ds(0, half), pl.ds(half, half))
    whole = pl.ds(0, rows)

    def pass_on(owner, h, to, recv):
        slot = seen_from(owner, to)
        remote(xs.at[owner, h], xs.at[slot, h], xs_send, recv, to).start()

    def send_own(i):
        pass_on(OWN, part[i], A0, half_recv.at[0, i])
        pass_on(OWN, part[1 - i], B0, half_recv.at[1, i])

    send_own(0)
    pass_on(OWN, whole, MATE, xs_recv.at[MATE])
    w_in = [pltpu.make_async_copy(wg_hbm, wgu.at[0], w_sem.at[0]), pltpu.make_async_copy(wu_hbm, wgu.at[1], w_sem.at[0]),
            pltpu.make_async_copy(wd_hbm, wd, w_sem.at[1])]

    pl.semaphore_wait(arrived.at[0], 2)
    pl.semaphore_signal(arrived.at[1], inc=1, device_id={"ep": dev[MATE]}, device_id_type=MESH)

    for cp in route_in:
        cp.wait()
    row8 = lax.broadcasted_iota(jnp.int32, (2 * n_exp, half), 0)
    in_first = row8 < n_exp
    exp_of = jnp.where(in_first, row8, row8 - n_exp)
    id_rep = [jnp.where(in_first, ids[j:j + 1, 0:half], ids[j:j + 1, half:rows]) for j in range(ids.shape[0])]
    g_rep = [jnp.where(in_first, gates[j:j + 1, 0:half], gates[j:j + 1, half:rows]) for j in range(ids.shape[0])]
    for s in range(8):
        want = exp_of + dev[s] * n_exp
        tab = jnp.zeros((2 * n_exp, half), F32)
        for j in range(ids.shape[0]):
            tab = tab + jnp.where(id_rep[j] == want, g_rep[j], 0.0)
        mytab[s] = tab
    tri[...] = (lax.broadcasted_iota(jnp.int32, (rows, rows), 0) <=
                lax.broadcasted_iota(jnp.int32, (rows, rows), 1)).astype(F32).astype(BF16)
    pl.semaphore_wait(arrived.at[1], 1)
    for s in range(1, 8):
        remote(mytab.at[s], tables.at[s], tab_send, tab_recv.at[s // 2], s).start()
    send_own(1)
    for cp in w_in:
        cp.start()

    def place(tab):
        hit = (tab != 0.0).astype(F32)
        one = [jnp.max(hit[i * n_exp:(i + 1) * n_exp], axis=0, keepdims=True) for i in range(2)]
        hit = jnp.concatenate(one, axis=1)
        count = jnp.dot(jnp.broadcast_to(hit, (16, rows)).astype(BF16), tri[...], preferred_element_type=F32)[0:1]
        return jnp.where(hit > 0.0, count - 1.0, -1.0)

    def one_hot(where):
        slot_row = lax.broadcasted_iota(jnp.int32, (half, rows), 0).astype(F32)
        return (slot_row == where).astype(F32)

    for s in range(8):
        rank_home[s:s + 1] = place(mytab[s])

    def tables_of(pair):
        wait_for(tables.at[pl.ds(pair[0], 2)] if pair[0] else tables.at[MATE], tab_recv.at[pair[0] // 2])

    def plan(pair):
        tables_of(pair)
        for slot in pair:
            tab = mytab[OWN] if slot == OWN else tables[slot]
            hot = one_hot(rank_home[OWN:OWN + 1] if slot == OWN else place(tab))
            pick[slot] = hot.astype(BF16)
            g = [lax.dot_general(hot[:, j * half:(j + 1) * half], tab, (((1,), (1,)), ((), ())),
                                 precision=lax.Precision.HIGHEST, preferred_element_type=F32) for j in range(2)]
            weight[slot] = g[0][:, 0:n_exp] + g[1][:, n_exp:2 * n_exp]

    def serve(pair, lo=0, count=half):
        these = pl.ds(lo, count)
        batch = row_in.at[pl.ds(0, 2 * count)]
        for i, slot in enumerate(pair):
            row_in[pl.ds(i * count, count), :] = jnp.dot(pick[slot, these], xs[slot], preferred_element_type=F32).astype(BF16)
        total = jnp.zeros(batch.shape, F32)
        for e in range(n_exp):
            a = jnp.dot(batch[...], wgu[0, e], preferred_element_type=F32)
            b = jnp.dot(batch[...], wgu[1, e], preferred_element_type=F32)
            hid = (a * (1.0 / (1.0 + jnp.exp(-a))) * b).astype(BF16)
            y = jnp.dot(hid, wd[e], preferred_element_type=F32).astype(BF16).astype(F32)
            g = jnp.concatenate([weight[slot, these, e:e + 1] for slot in pair], axis=0)
            total = total + jnp.where(g != 0.0, g * y, 0.0)
        total = total.astype(BF16)
        for i, slot in enumerate(pair):
            (home if slot == OWN else sums)[slot, these] = total[i * count:(i + 1) * count]
        for slot in pair:
            if slot != OWN:
                remote(sums.at[slot, these], home.at[slot, these], s_send, s_recv.at[4 if slot == O1 else slot // 2], slot).start()

    for slot, on, i in ((A0, B0, 0), (B0, A0, 1)):
        wait_for(xs.at[slot, part[i]], half_recv.at[i, 0])
        pass_on(slot, part[i], on, xs_recv.at[O0])
        pass_on(slot, part[i], MATE, xs_recv.at[seen_from(slot, MATE)])
    for pair in ((A0, B0), (A1, B1), (O0, O1), (OWN, MATE)):
        plan(pair)
    wait_for(wgu, w_sem.at[0])
    w_in[2].wait()
    for slot, i in ((A0, 0), (B0, 1)):
        wait_for(xs.at[slot, part[1 - i]], half_recv.at[i, 1])
        pass_on(slot, part[1 - i], MATE, xs_recv.at[seen_from(slot, MATE)])
    for lo in (0, half // 2):
        serve((A0, B0), lo, half // 2)
    wait_for(xs.at[A1], xs_recv.at[A1])
    wait_for(xs.at[B1], xs_recv.at[B1])
    serve((A1, B1))
    wait_for(xs.at[O0], xs_recv.at[O0])
    pass_on(O0, whole, MATE, xs_recv.at[O1])
    wait_for(xs.at[O1], xs_recv.at[O1])
    serve((O0, O1))
    wait_for(xs.at[MATE], xs_recv.at[MATE])
    serve((OWN, MATE))

    def back_home(*slots):
        hot = jnp.concatenate([one_hot(rank_home[s:s + 1]) for s in slots], axis=0).astype(BF16)
        got = home[pl.ds(slots[0], len(slots))].reshape(hot.shape[0], home.shape[2])
        return lax.dot_general(hot, got, (((0,), (0,)), ((), ())), preferred_element_type=F32)

    wait_for(home.at[MATE], s_recv.at[0])
    acc[...] = xs[OWN].astype(F32) + back_home(OWN, MATE)
    for pair in (A0, A1):
        wait_for(home.at[pl.ds(pair, 2)], s_recv.at[pair // 2])
        acc[...] += back_home(pair, pair + 1)
    wait_for(home.at[O0], s_recv.at[O0 // 2])
    acc[...] += back_home(O0)
    wait_for(home.at[O1], s_recv.at[4])
    out[...] = (acc[...] + back_home(O1)).astype(BF16)
    for ref, sem in ((xs, xs_send), (mytab, tab_send), (sums, s_send)):
        remote(ref.at[pl.ds(0, 7)], ref.at[pl.ds(0, 7)], sem, s_recv.at[0], MATE).wait_send()


def solution(mesh):
    row_spec = P(('dp', 'ep'))
    expert_spec = P('ep')
    group = mesh.shape['ep']
    assert group == 8

    def device_step(tokens, expert_ids, gate_vals, w_gate, w_up, w_down):
        rows, width = tokens.shape
        n_exp, _, hidden = w_gate.shape
        half = rows // 2
        in_hbm = functools.partial(pltpu.with_memory_space_constraint, memory_space=pltpu.HBM)
        dma = pltpu.SemaphoreType.DMA
        return pl.pallas_call(
            kernel,
            out_shape=jax.ShapeDtypeStruct((rows, width), BF16),
            in_specs=[pl.BlockSpec(memory_space=pltpu.HBM)] * 6,
            out_specs=pl.BlockSpec(memory_space=pltpu.VMEM),
            scratch_shapes=[
                pltpu.VMEM((group, rows, width), BF16),
                pltpu.VMEM((group, 2 * n_exp, half), F32),
                pltpu.VMEM((group, 2 * n_exp, half), F32),
                pltpu.VMEM((rows, rows), BF16),
                pltpu.VMEM((2, n_exp, width, hidden), BF16),
                pltpu.VMEM((n_exp, hidden, width), BF16),
                pltpu.VMEM((rows, width), BF16),
                pltpu.VMEM((group, half, width), BF16),
                pltpu.VMEM((group, half, width), BF16),
                pltpu.VMEM((rows, width), F32),
                pltpu.VMEM((group, rows), F32),
                pltpu.VMEM((expert_ids.shape[1], rows), jnp.int32),
                pltpu.VMEM((expert_ids.shape[1], rows), F32),
                pltpu.VMEM((group, half, rows), BF16),
                pltpu.VMEM((group, half, n_exp), F32),
                dma, dma((2,)), dma((2,)), dma, dma, dma, dma((group,)), dma((2, 2)), dma((4,)), dma((5,)),
                pltpu.SemaphoreType.REGULAR((2,)),
            ],
            compiler_params=pltpu.CompilerParams(collective_id=0, has_side_effects=True, vmem_limit_bytes=40 * 1024 * 1024),
        )(*map(in_hbm, (tokens, expert_ids.T, gate_vals.T, w_gate, w_up, w_down)))

    return jax.shard_map(device_step, mesh=mesh, in_specs=(row_spec, row_spec, row_spec, expert_spec, expert_spec, expert_spec),
                         out_specs=row_spec, check_vma=False)
```

```python
import functools

import jax
import jax.numpy as jnp
from jax import lax
from jax.experimental import pallas as pl
from jax.experimental.pallas import tpu as pltpu
from jax.sharding import PartitionSpec as P

MESH = pl.DeviceIdType.MESH
F32, BF16 = jnp.float32, jnp.bfloat16
OWN, MATE, A0, B0, A1, B1, O0, O1 = range(8)
CHIP = (0, 0, 1, 3, 1, 3, 2, 2)
CORE = (0, 1, 0, 0, 1, 1, 0, 1)


def seen_from(owner, reader):
    want = (CHIP[owner] ^ CHIP[reader], CORE[owner] ^ CORE[reader])
    return [s for s in range(8) if (CHIP[s], CORE[s]) == want][0]


def kernel(tok, ids_hbm, gates_hbm, wg_hbm, wu_hbm, wd_hbm, out,
           xs, tables, mytab, tri, wgu, wd, row_in, sums, home, acc, rank_home, ids, gates, pick, weight, home_near, pick_near,
           tok_sem, route_sem, w_sem, xs_send, tab_send, s_send, xs_recv, half_recv, tab_recv, s_recv, arrived,
           relay, relay_send, relay_recv):
    rows, half = tok.shape[0], tok.shape[0] // 2
    n_exp = wd.shape[0]
    me = lax.axis_index("ep")
    x = me // 2
    c = me - 2 * x
    x_of = (x, x + 1 - 2 * lax.rem(x, 2), lax.rem(x + 2, 4), 3 - x)
    dev = [2 * x_of[CHIP[s]] + (1 - c if CORE[s] else c) for s in range(8)]

    def remote(src, dst, send, recv, slot):
        return pltpu.make_async_remote_copy(src_ref=src, dst_ref=dst, send_sem=send, recv_sem=recv,
                                            device_id={"ep": dev[slot]}, device_id_type=MESH)

    def wait_for(ref, sem):
        remote(ref, ref, xs_send, sem, MATE).wait_recv()

    barrier = pltpu.get_barrier_semaphore()
    for s in (A0, B0, MATE):
        pl.semaphore_signal(barrier, inc=1, device_id={"ep": dev[s]}, device_id_type=MESH)
    tok_in = pltpu.make_async_copy(tok, xs.at[OWN], tok_sem)
    tok_in.start()
    route_in = [pltpu.make_async_copy(h, v, route_sem.at[i]) for i, (h, v) in enumerate(((ids_hbm, ids), (gates_hbm, gates)))]
    for cp in route_in:
        cp.start()
    pl.semaphore_wait(barrier, 3)
    for s in (A0, B0):
        pl.semaphore_signal(arrived.at[0], inc=1, device_id={"ep": dev[s]}, device_id_type=MESH)
    tok_in.wait()

    part = (pl.ds(0, half), pl.ds(half, half))
    whole = pl.ds(0, rows)

    def pass_on(owner, h, to, recv):
        slot = seen_from(owner, to)
        remote(xs.at[owner, h], xs.at[slot, h], xs_send, recv, to).start()

    def send_own(i):
        pass_on(OWN, part[i], A0, half_recv.at[0, i])
        pass_on(OWN, part[1 - i], B0, half_recv.at[1, i])

    send_own(0)
    pass_on(OWN, whole, MATE, xs_recv.at[MATE])
    w_in = [pltpu.make_async_copy(wg_hbm, wgu.at[0], w_sem.at[0]), pltpu.make_async_copy(wu_hbm, wgu.at[1], w_sem.at[0]),
            pltpu.make_async_copy(wd_hbm, wd, w_sem.at[1])]

    pl.semaphore_wait(arrived.at[0], 2)
    pl.semaphore_signal(arrived.at[1], inc=1, device_id={"ep": dev[MATE]}, device_id_type=MESH)

    for cp in route_in:
        cp.wait()
    row8 = lax.broadcasted_iota(jnp.int32, (2 * n_exp, half), 0)
    in_first = row8 < n_exp
    exp_of = jnp.where(in_first, row8, row8 - n_exp)
    id_rep = [jnp.where(in_first, ids[j:j + 1, 0:half], ids[j:j + 1, half:rows]) for j in range(ids.shape[0])]
    g_rep = [jnp.where(in_first, gates[j:j + 1, 0:half], gates[j:j + 1, half:rows]) for j in range(ids.shape[0])]
    for s in range(8):
        want = exp_of + dev[s] * n_exp
        tab = jnp.zeros((2 * n_exp, half), F32)
        for j in range(ids.shape[0]):
            tab = tab + jnp.where(id_rep[j] == want, g_rep[j], 0.0)
        mytab[s] = tab
    tri[...] = (lax.broadcasted_iota(jnp.int32, (rows, rows), 0) <=
                lax.broadcasted_iota(jnp.int32, (rows, rows), 1)).astype(F32).astype(BF16)
    pl.semaphore_wait(arrived.at[1], 1)
    for s in range(1, 8):
        remote(mytab.at[s], tables.at[s], tab_send, tab_recv.at[s // 2], s).start()
    send_own(1)
    for cp in w_in:
        cp.start()

    def place(tab):
        hit = (tab != 0.0).astype(F32)
        one = [jnp.max(hit[i * n_exp:(i + 1) * n_exp], axis=0, keepdims=True) for i in range(2)]
        hit = jnp.concatenate(one, axis=1)
        count = jnp.dot(jnp.broadcast_to(hit, (16, rows)).astype(BF16), tri[...], preferred_element_type=F32)[0:1]
        return jnp.where(hit > 0.0, count - 1.0, -1.0)

    def one_hot(where):
        slot_row = lax.broadcasted_iota(jnp.int32, (half, rows), 0).astype(F32)
        return (slot_row == where).astype(F32)

    for s in range(8):
        rank_home[s:s + 1] = place(mytab[s])

    def tables_of(pair):
        wait_for(tables.at[pl.ds(pair[0], 2)] if pair[0] else tables.at[MATE], tab_recv.at[pair[0] // 2])

    def plan(pair):
        tables_of(pair)
        for slot in pair:
            tab = mytab[OWN] if slot == OWN else tables[slot]
            hot = one_hot(rank_home[OWN:OWN + 1] if slot == OWN else place(tab))
            pick[slot] = hot.astype(BF16)
            g = [lax.dot_general(hot[:, j * half:(j + 1) * half], tab, (((1,), (1,)), ((), ())),
                                 precision=lax.Precision.HIGHEST, preferred_element_type=F32) for j in range(2)]
            weight[slot] = g[0][:, 0:n_exp] + g[1][:, n_exp:2 * n_exp]

    quarter = (pl.ds(0, half // 2), pl.ds(half // 2, half // 2))

    def first_hop(slot):
        for i, by in enumerate((A0, B0)):
            remote(sums.at[slot, quarter[i]], relay.at[i, slot - O0], s_send, relay_recv.at[i, slot - O0], by).start()

    def second_hop(slot):
        for i, to in enumerate((B0, A0)):
            wait_for(relay.at[i, slot - O0], relay_recv.at[i, slot - O0])
            remote(relay.at[i, slot - O0], home.at[slot, quarter[i]], relay_send, s_recv.at[O0 // 2],
                   to if slot == O0 else seen_from(to, MATE)).start()

    def serve(pair, lo=0, count=half):
        these = pl.ds(lo, count)
        batch = row_in.at[pl.ds(0, len(pair) * count)]
        for i, slot in enumerate(pair):
            row_in[pl.ds(i * count, count), :] = jnp.dot(pick[slot, these], xs[slot], preferred_element_type=F32).astype(BF16)
        total = jnp.zeros(batch.shape, F32)
        for e in range(n_exp):
            a = jnp.dot(batch[...], wgu[0, e], preferred_element_type=F32)
            b = jnp.dot(batch[...], wgu[1, e], preferred_element_type=F32)
            hid = (a * (1.0 / (1.0 + jnp.exp(-a))) * b).astype(BF16)
            y = jnp.dot(hid, wd[e], preferred_element_type=F32).astype(BF16).astype(F32)
            g = jnp.concatenate([weight[slot, these, e:e + 1] for slot in pair], axis=0)
            total = total + jnp.where(g != 0.0, g * y, 0.0)
        total = total.astype(BF16)
        for i, slot in enumerate(pair):
            (home if slot is OWN else sums)[slot, these] = total[i * count:(i + 1) * count]

    for slot, on, i in ((A0, B0, 0), (B0, A0, 1)):
        wait_for(xs.at[slot, part[i]], half_recv.at[i, 0])
        pass_on(slot, part[i], on, xs_recv.at[O0])
        pass_on(slot, part[i], MATE, xs_recv.at[seen_from(slot, MATE)])
    for pair in ((A0, B0), (A1, B1), (O0, O1), (OWN, MATE)):
        plan(pair)
    wait_for(wgu, w_sem.at[0])
    w_in[2].wait()
    for slot, i in ((A0, 0), (B0, 1)):
        wait_for(xs.at[slot, part[1 - i]], half_recv.at[i, 1])
        pass_on(slot, part[1 - i], MATE, xs_recv.at[seen_from(slot, MATE)])
    ones = [A0 + 2 * (1 - c), B0 + 2 * (1 - c)]
    zeros = [A0 + 2 * c, B0 + 2 * c]

    def serve_neighbours(pair, core, i):
        serve(pair, i * half // 2, half // 2)

    def answer_neighbours(pair, core, i):
        for slot, chip in zip(pair, (CHIP[A0], CHIP[B0])):
            pltpu.make_async_remote_copy(src_ref=sums.at[slot, quarter[i]], dst_ref=home_near.at[i, slot - A0],
                                         send_sem=s_send, recv_sem=s_recv.at[1 + i],
                                         device_id={"ep": 2 * x_of[chip] + core}, device_id_type=MESH).start()

    first, early, late, last = ([A0, B0], c, 0), (ones, 1, 1), ([A1, B1], 1 - c, 0), (zeros, 0, 1)
    serve_neighbours(*first)
    answer_neighbours(*first)
    wait_for(xs.at[A1], xs_recv.at[A1])
    wait_for(xs.at[B1], xs_recv.at[B1])
    serve_neighbours(*early)
    answer_neighbours(*early)
    wait_for(xs.at[O0], xs_recv.at[O0])
    pass_on(O0, whole, MATE, xs_recv.at[O1])
    serve([O0])
    first_hop(O0)
    wait_for(xs.at[O1], xs_recv.at[O1])
    serve([O1])
    first_hop(O1)
    for rest, slot in ((late, O0), (last, O1)):
        serve_neighbours(*rest)
        second_hop(slot)
    answer_neighbours(*late)
    answer_neighbours(*last)
    wait_for(xs.at[MATE], xs_recv.at[MATE])
    serve([OWN, MATE])
    remote(sums.at[MATE], home.at[MATE], s_send, s_recv.at[0], MATE).start()

    def back_home(*slots):
        hot = jnp.concatenate([one_hot(rank_home[s:s + 1]) for s in slots], axis=0).astype(BF16)
        got = home[pl.ds(slots[0], len(slots))].reshape(hot.shape[0], home.shape[2])
        return lax.dot_general(hot, got, (((0,), (0,)), ((), ())), preferred_element_type=F32)

    wait_for(home.at[MATE], s_recv.at[0])
    acc[...] = xs[OWN].astype(F32) + back_home(OWN, MATE)
    square = (rows, rows)
    eye = (lax.broadcasted_iota(jnp.int32, square, 0) == lax.broadcasted_iota(jnp.int32, square, 1)).astype(F32).astype(BF16)
    near = [one_hot(rank_home[s:s + 1]) for s in (A0, B0, A1, B1)]
    for i in range(2):
        hot = jnp.concatenate([h[i * half // 2:(i + 1) * half // 2] for h in near], axis=0).astype(BF16)
        pick_near[i] = lax.dot_general(hot, eye, (((0,), (0,)), ((), ())), preferred_element_type=F32).astype(BF16)

    def near_sum(i):
        return jnp.dot(pick_near[i], home_near[i].reshape(rows, home.shape[2]), preferred_element_type=F32)

    wait_for(home.at[pl.ds(O0, 2)], s_recv.at[3])
    acc[...] += back_home(O0, O1)
    wait_for(home_near.at[0], s_recv.at[1])
    acc[...] += near_sum(0)
    for ref, sem in ((xs, xs_send), (mytab, tab_send), (sums, s_send)):
        remote(ref.at[pl.ds(0, 7)], ref.at[pl.ds(0, 7)], sem, s_recv.at[0], MATE).wait_send()
    remote(relay, relay, relay_send, s_recv.at[0], MATE).wait_send()
    wait_for(home_near.at[1], s_recv.at[2])
    out[...] = (acc[...] + near_sum(1)).astype(BF16)


def solution(mesh):
    row_spec = P(('dp', 'ep'))
    expert_spec = P('ep')
    group = mesh.shape['ep']
    assert group == 8

    def device_step(tokens, expert_ids, gate_vals, w_gate, w_up, w_down):
        rows, width = tokens.shape
        n_exp, _, hidden = w_gate.shape
        half = rows // 2
        in_hbm = functools.partial(pltpu.with_memory_space_constraint, memory_space=pltpu.HBM)
        dma = pltpu.SemaphoreType.DMA
        return pl.pallas_call(
            kernel,
            out_shape=jax.ShapeDtypeStruct((rows, width), BF16),
            in_specs=[pl.BlockSpec(memory_space=pltpu.HBM)] * 6,
            out_specs=pl.BlockSpec(memory_space=pltpu.VMEM),
            scratch_shapes=[
                pltpu.VMEM((group, rows, width), BF16),
                pltpu.VMEM((group, 2 * n_exp, half), F32),
                pltpu.VMEM((group, 2 * n_exp, half), F32),
                pltpu.VMEM((rows, rows), BF16),
                pltpu.VMEM((2, n_exp, width, hidden), BF16),
                pltpu.VMEM((n_exp, hidden, width), BF16),
                pltpu.VMEM((rows, width), BF16),
                pltpu.VMEM((group, half, width), BF16),
                pltpu.VMEM((group, half, width), BF16),
                pltpu.VMEM((rows, width), F32),
                pltpu.VMEM((group, rows), F32),
                pltpu.VMEM((expert_ids.shape[1], rows), jnp.int32),
                pltpu.VMEM((expert_ids.shape[1], rows), F32),
                pltpu.VMEM((group, half, rows), BF16),
                pltpu.VMEM((group, half, n_exp), F32),
                pltpu.VMEM((2, 4, half // 2, width), BF16),
                pltpu.VMEM((2, rows, rows), BF16),
                dma, dma((2,)), dma((2,)), dma, dma, dma, dma((group,)), dma((2, 2)), dma((4,)), dma((4,)),
                pltpu.SemaphoreType.REGULAR((2,)),
                pltpu.VMEM((2, 2, half // 2, width), BF16),
                dma, dma((2, 2)),
            ],
            compiler_params=pltpu.CompilerParams(collective_id=0, has_side_effects=True, vmem_limit_bytes=40 * 1024 * 1024),
        )(*map(in_hbm, (tokens, expert_ids.T, gate_vals.T, w_gate, w_up, w_down)))

    return jax.shard_map(device_step, mesh=mesh, in_specs=(row_spec, row_spec, row_spec, expert_spec, expert_spec, expert_spec),
                         out_specs=row_spec, check_vma=False)
```

```python
import functools

import jax
import jax.numpy as jnp
from jax import lax
from jax.experimental import pallas as pl
from jax.experimental.pallas import tpu as pltpu
from jax.sharding import PartitionSpec as P

MESH = pl.DeviceIdType.MESH
F32, BF16 = jnp.float32, jnp.bfloat16
OWN, MATE, A0, B0, A1, B1, O0, O1 = range(8)
CHIP = (0, 0, 1, 3, 1, 3, 2, 2)
CORE = (0, 1, 0, 0, 1, 1, 0, 1)


def seen_from(owner, reader):
    want = (CHIP[owner] ^ CHIP[reader], CORE[owner] ^ CORE[reader])
    return [s for s in range(8) if (CHIP[s], CORE[s]) == want][0]


def kernel(tok, ids_hbm, gates_hbm, wg_hbm, wu_hbm, wd_hbm, out,
           xs, tables, mytab, tri, wgu, wd, row_in, sums, home, acc, rank_home, ids, gates, pick, weight, home_near, pick_near,
           tok_sem, route_sem, w_sem, xs_send, tab_send, s_send, xs_recv, half_recv, tab_recv, s_recv, arrived,
           relay, relay_send, relay_recv):
    rows, half = tok.shape[0], tok.shape[0] // 2
    n_exp = wd.shape[0]
    me = lax.axis_index("ep")
    x = me // 2
    c = me - 2 * x
    x_of = (x, x + 1 - 2 * lax.rem(x, 2), lax.rem(x + 2, 4), 3 - x)
    dev = [2 * x_of[CHIP[s]] + (1 - c if CORE[s] else c) for s in range(8)]

    def remote(src, dst, send, recv, slot):
        return pltpu.make_async_remote_copy(src_ref=src, dst_ref=dst, send_sem=send, recv_sem=recv,
                                            device_id={"ep": dev[slot]}, device_id_type=MESH)

    def wait_for(ref, sem):
        remote(ref, ref, xs_send, sem, MATE).wait_recv()

    barrier = pltpu.get_barrier_semaphore()
    for s in (A0, B0, MATE):
        pl.semaphore_signal(barrier, inc=1, device_id={"ep": dev[s]}, device_id_type=MESH)
    tok_in = pltpu.make_async_copy(tok, xs.at[OWN], tok_sem)
    tok_in.start()
    route_in = [pltpu.make_async_copy(h, v, route_sem.at[i]) for i, (h, v) in enumerate(((ids_hbm, ids), (gates_hbm, gates)))]
    for cp in route_in:
        cp.start()
    pl.semaphore_wait(barrier, 3)
    for s in (A0, B0):
        pl.semaphore_signal(arrived.at[0], inc=1, device_id={"ep": dev[s]}, device_id_type=MESH)
    tok_in.wait()

    part = (pl.ds(0, half), pl.ds(half, half))
    whole = pl.ds(0, rows)

    def block_sem(slot):
        return xs_recv.at[{MATE: 0, A1: 1, B1: 1, O0: 2, O1: 3}[slot]]

    def pass_on(owner, h, to, recv):
        slot = seen_from(owner, to)
        remote(xs.at[owner, h], xs.at[slot, h], xs_send, recv, to).start()

    def send_own(i):
        pass_on(OWN, part[i], A0, half_recv.at[0, i])
        pass_on(OWN, part[1 - i], B0, half_recv.at[1, i])

    send_own(0)
    pass_on(OWN, whole, MATE, block_sem(MATE))
    w_in = [pltpu.make_async_copy(wg_hbm, wgu.at[0], w_sem.at[0]), pltpu.make_async_copy(wu_hbm, wgu.at[1], w_sem.at[0]),
            pltpu.make_async_copy(wd_hbm, wd, w_sem.at[1])]

    pl.semaphore_wait(arrived.at[0], 2)
    pl.semaphore_signal(arrived.at[1], inc=1, device_id={"ep": dev[MATE]}, device_id_type=MESH)

    for cp in route_in:
        cp.wait()
    row8 = lax.broadcasted_iota(jnp.int32, (2 * n_exp, half), 0)
    in_first = row8 < n_exp
    exp_of = jnp.where(in_first, row8, row8 - n_exp)
    id_rep = [jnp.where(in_first, ids[j:j + 1, 0:half], ids[j:j + 1, half:rows]) for j in range(ids.shape[0])]
    g_rep = [jnp.where(in_first, gates[j:j + 1, 0:half], gates[j:j + 1, half:rows]) for j in range(ids.shape[0])]
    for s in range(8):
        want = exp_of + dev[s] * n_exp
        tab = jnp.zeros((2 * n_exp, half), F32)
        for j in range(ids.shape[0]):
            tab = tab + jnp.where(id_rep[j] == want, g_rep[j], 0.0)
        mytab[s] = tab
    tri[...] = (lax.broadcasted_iota(jnp.int32, (rows, rows), 0) <=
                lax.broadcasted_iota(jnp.int32, (rows, rows), 1)).astype(F32).astype(BF16)
    pl.semaphore_wait(arrived.at[1], 1)
    for s in range(1, 8):
        remote(mytab.at[s], tables.at[s], tab_send, tab_recv, s).start()
    send_own(1)
    for cp in w_in:
        cp.start()

    def place(tab):
        hit = (tab != 0.0).astype(F32)
        one = [jnp.max(hit[i * n_exp:(i + 1) * n_exp], axis=0, keepdims=True) for i in range(2)]
        hit = jnp.concatenate(one, axis=1)
        count = jnp.dot(jnp.broadcast_to(hit, (16, rows)).astype(BF16), tri[...], preferred_element_type=F32)[0:1]
        return jnp.where(hit > 0.0, count - 1.0, -1.0)

    def one_hot(where):
        slot_row = lax.broadcasted_iota(jnp.int32, (half, rows), 0).astype(F32)
        return (slot_row == where).astype(F32)

    for s in range(8):
        rank_home[s:s + 1] = place(mytab[s])

    def plan(pair):
        for slot in pair:
            tab = mytab[OWN] if slot == OWN else tables[slot]
            hot = one_hot(rank_home[OWN:OWN + 1] if slot == OWN else place(tab))
            pick[slot] = hot.astype(BF16)
            g = [lax.dot_general(hot[:, j * half:(j + 1) * half], tab, (((1,), (1,)), ((), ())),
                                 precision=lax.Precision.HIGHEST, preferred_element_type=F32) for j in range(2)]
            weight[slot] = g[0][:, 0:n_exp] + g[1][:, n_exp:2 * n_exp]

    quarter = (pl.ds(0, half // 2), pl.ds(half // 2, half // 2))

    def first_hop(slot):
        for i, by in enumerate((A0, B0)):
            remote(sums.at[slot, quarter[i]], relay.at[slot - O0, i], s_send, relay_recv.at[slot - O0, i], by).start()

    def second_hop(slot):
        for i, to in enumerate((B0, A0)):
            wait_for(relay.at[slot - O0, i], relay_recv.at[slot - O0, i])
            remote(relay.at[slot - O0, i], home.at[slot, quarter[i]], relay_send, s_recv.at[O0 // 2],
                   to if slot == O0 else seen_from(to, MATE)).start()

    def serve(pair, lo=0, count=half):
        these = pl.ds(lo, count)
        batch = row_in.at[pl.ds(0, len(pair) * count)]
        for i, slot in enumerate(pair):
            row_in[pl.ds(i * count, count), :] = jnp.dot(pick[slot, these], xs[slot], preferred_element_type=F32).astype(BF16)
        total = jnp.zeros(batch.shape, F32)
        for e in range(n_exp):
            a = jnp.dot(batch[...], wgu[0, e], preferred_element_type=F32)
            b = jnp.dot(batch[...], wgu[1, e], preferred_element_type=F32)
            hid = (a * (1.0 / (1.0 + jnp.exp(-a))) * b).astype(BF16)
            y = jnp.dot(hid, wd[e], preferred_element_type=F32).astype(BF16).astype(F32)
            g = jnp.concatenate([weight[slot, these, e:e + 1] for slot in pair], axis=0)
            total = total + jnp.where(g != 0.0, g * y, 0.0)
        total = total.astype(BF16)
        for i, slot in enumerate(pair):
            (home if slot is OWN else sums)[slot, these] = total[i * count:(i + 1) * count]

    for slot, on, i in ((A0, B0, 0), (B0, A0, 1)):
        wait_for(xs.at[slot, part[i]], half_recv.at[i, 0])
        pass_on(slot, part[i], on, block_sem(O0))
        pass_on(slot, part[i], MATE, block_sem(seen_from(slot, MATE)))
    wait_for(tables.at[pl.ds(1, 7)], tab_recv)
    for pair in ((A0, B0), (A1, B1), (O0, O1), (OWN, MATE)):
        plan(pair)
    wait_for(wgu, w_sem.at[0])
    w_in[2].wait()
    for slot, i in ((A0, 0), (B0, 1)):
        wait_for(xs.at[slot, part[1 - i]], half_recv.at[i, 1])
        pass_on(slot, part[1 - i], MATE, block_sem(seen_from(slot, MATE)))
    ones = [A0 + 2 * (1 - c), B0 + 2 * (1 - c)]
    zeros = [A0 + 2 * c, B0 + 2 * c]

    def serve_neighbours(pair, core, i):
        serve(pair, i * half // 2, half // 2)

    def answer_neighbours(pair, core, i):
        for slot, chip in zip(pair, (CHIP[A0], CHIP[B0])):
            pltpu.make_async_remote_copy(src_ref=sums.at[slot, quarter[i]], dst_ref=home_near.at[i, slot - A0],
                                         send_sem=s_send, recv_sem=s_recv.at[1 + i],
                                         device_id={"ep": 2 * x_of[chip] + core}, device_id_type=MESH).start()

    first, early, late, last = ([A0, B0], c, 0), (ones, 1, 1), ([A1, B1], 1 - c, 0), (zeros, 0, 1)
    serve_neighbours(*first)
    answer_neighbours(*first)
    wait_for(xs.at[pl.ds(A1, 2)], block_sem(A1))
    serve_neighbours(*early)
    answer_neighbours(*early)
    wait_for(xs.at[O0], block_sem(O0))
    pass_on(O0, whole, MATE, block_sem(O1))
    serve([O0])
    first_hop(O0)
    wait_for(xs.at[O1], block_sem(O1))
    serve([O1])
    first_hop(O1)
    for rest, slot in ((late, O0), (last, O1)):
        serve_neighbours(*rest)
        second_hop(slot)
    answer_neighbours(*late)
    answer_neighbours(*last)
    wait_for(xs.at[MATE], block_sem(MATE))
    serve([OWN, MATE])
    remote(sums.at[MATE], home.at[MATE], s_send, s_recv.at[0], MATE).start()

    def back_home(*slots):
        hot = jnp.concatenate([one_hot(rank_home[s:s + 1]) for s in slots], axis=0).astype(BF16)
        got = home[pl.ds(slots[0], len(slots))].reshape(hot.shape[0], home.shape[2])
        return lax.dot_general(hot, got, (((0,), (0,)), ((), ())), preferred_element_type=F32)

    wait_for(home.at[MATE], s_recv.at[0])
    acc[...] = xs[OWN].astype(F32) + back_home(OWN, MATE)
    square = (rows, rows)
    eye = (lax.broadcasted_iota(jnp.int32, square, 0) == lax.broadcasted_iota(jnp.int32, square, 1)).astype(F32).astype(BF16)
    near = [one_hot(rank_home[s:s + 1]) for s in (A0, B0, A1, B1)]
    for i in range(2):
        hot = jnp.concatenate([h[i * half // 2:(i + 1) * half // 2] for h in near], axis=0).astype(BF16)
        pick_near[i] = lax.dot_general(hot, eye, (((0,), (0,)), ((), ())), preferred_element_type=F32).astype(BF16)

    def near_sum(i):
        return jnp.dot(pick_near[i], home_near[i].reshape(rows, home.shape[2]), preferred_element_type=F32)

    wait_for(home.at[pl.ds(O0, 2)], s_recv.at[3])
    acc[...] += back_home(O0, O1)
    wait_for(home_near.at[0], s_recv.at[1])
    acc[...] += near_sum(0)
    for ref, sem in ((xs, xs_send), (mytab, tab_send), (sums, s_send)):
        remote(ref.at[pl.ds(0, 7)], ref.at[pl.ds(0, 7)], sem, s_recv.at[0], MATE).wait_send()
    remote(relay, relay, relay_send, s_recv.at[0], MATE).wait_send()
    wait_for(home_near.at[1], s_recv.at[2])
    out[...] = (acc[...] + near_sum(1)).astype(BF16)


def solution(mesh):
    row_spec = P(('dp', 'ep'))
    expert_spec = P('ep')
    group = mesh.shape['ep']
    assert group == 8

    def device_step(tokens, expert_ids, gate_vals, w_gate, w_up, w_down):
        rows, width = tokens.shape
        n_exp, _, hidden = w_gate.shape
        half = rows // 2
        in_hbm = functools.partial(pltpu.with_memory_space_constraint, memory_space=pltpu.HBM)
        dma = pltpu.SemaphoreType.DMA
        return pl.pallas_call(
            kernel,
            out_shape=jax.ShapeDtypeStruct((rows, width), BF16),
            in_specs=[pl.BlockSpec(memory_space=pltpu.HBM)] * 6,
            out_specs=pl.BlockSpec(memory_space=pltpu.VMEM),
            scratch_shapes=[
                pltpu.VMEM((group, rows, width), BF16),
                pltpu.VMEM((group, 2 * n_exp, half), F32),
                pltpu.VMEM((group, 2 * n_exp, half), F32),
                pltpu.VMEM((rows, rows), BF16),
                pltpu.VMEM((2, n_exp, width, hidden), BF16),
                pltpu.VMEM((n_exp, hidden, width), BF16),
                pltpu.VMEM((rows, width), BF16),
                pltpu.VMEM((group, half, width), BF16),
                pltpu.VMEM((group, half, width), BF16),
                pltpu.VMEM((rows, width), F32),
                pltpu.VMEM((group, rows), F32),
                pltpu.VMEM((expert_ids.shape[1], rows), jnp.int32),
                pltpu.VMEM((expert_ids.shape[1], rows), F32),
                pltpu.VMEM((group, half, rows), BF16),
                pltpu.VMEM((group, half, n_exp), F32),
                pltpu.VMEM((2, 4, half // 2, width), BF16),
                pltpu.VMEM((2, rows, rows), BF16),
                dma, dma((2,)), dma((2,)), dma, dma, dma, dma((4,)), dma((2, 2)), dma, dma((4,)),
                pltpu.SemaphoreType.REGULAR((2,)),
                pltpu.VMEM((2, 2, half // 2, width), BF16),
                dma, dma((2, 2)),
            ],
            compiler_params=pltpu.CompilerParams(collective_id=0, has_side_effects=True, vmem_limit_bytes=40 * 1024 * 1024),
        )(*map(in_hbm, (tokens, expert_ids.T, gate_vals.T, w_gate, w_up, w_down)))

    return jax.shard_map(device_step, mesh=mesh, in_specs=(row_spec, row_spec, row_spec, expert_spec, expert_spec, expert_spec),
                         out_specs=row_spec, check_vma=False)
```
